32 devices in a mesh: seq: 8 (over z, core), ch: 4 (over y, x).
Axes of the slice: x: 2, y: 2, z: 4, core: 2. Of those that a mesh axis runs over, the one named last changes fastest.
Arguments:
- input_q: bfloat16 [4096, 8192], P('seq', 'ch'), may hold values from -6 to 6
- input_k: bfloat16 [4096, 8192], P('seq', 'ch'), may hold values from -6 to 6
- input_v: bfloat16 [4096, 8192], P('seq', 'ch'), may hold values from -6 to 6
- grad_out: bfloat16 [4096, 8192], P('seq', 'ch'), may hold values from -6 to 6
- short_filters: float32 [3, 3, 8192], P(None, None, 'ch'), may hold values from -3.5 to 3.5
- long_filter: float32 [128, 8192], P(None, 'ch'), may hold values from -0.5 to 0.5
- skip_gain: float32 [8192], P('ch'), may hold values from 0.5 to 1.5
Outputs:
- grad_input_q: bfloat16 [4096, 8192], P('seq', 'ch')
- grad_input_k: bfloat16 [4096, 8192], P('seq', 'ch')
- grad_input_v: bfloat16 [4096, 8192], P('seq', 'ch')
- grad_long: float32 [128, 8192], P('seq', 'ch')
- grad_short: float32 [3, 3, 8192], P(None, None, 'ch')
- grad_skip: float32 [8192], P('ch')
The draws below stay inside these ranges and needn't reach their ends.
All inputs are finite; a program needn't handle non-finite values.
Results may differ from the reference program's by a relative error of at most 0.001.
Values may be sent and summed in bfloat16 or wider, within the bound.
A program may use at most 128 MiB of HBM per device.

```python
import math
import jax
import jax.numpy as jnp
from jax import lax

D = 8192
TAPS = 3
FILT = 128
SEQ = 4096


def levels(stream_key, shape, shards, smallest, high):
    level, own = 1.0, jax.random.fold_in(stream_key, 6)
    for axis_at, shards_of in shards:
        draws = jnp.exp(jax.random.uniform(jax.random.fold_in(own, axis_at), (shards_of,), jnp.float32, smallest / len(shards), high / len(shards)))
        level = level * jnp.repeat(draws, shape[axis_at] // shards_of).reshape([-1 if axis == axis_at else 1 for axis in range(len(shape))])
    return level


def gaussian(key, dims, scale, limit, cuts=(), dtype=jnp.bfloat16):
    factor_of = levels(key, dims, cuts, -0.22, 0.18) if cuts else 1.0
    entries = jax.random.normal(key, dims, jnp.float32) * scale * factor_of
    return jnp.minimum(jnp.maximum(entries, -limit), limit).astype(dtype)


def setup_inputs(seed: int = 0) -> dict:
    arg_keys = jax.random.split(jax.random.key(seed), 8)
    return {
        "input_q": gaussian(arg_keys[0], (SEQ, D), 1.0, 6.0, ((0, 8), (1, 4))),
        "input_k": gaussian(arg_keys[1], (SEQ, D), 1.0, 6.0, ((0, 8), (1, 4))),
        "input_v": gaussian(arg_keys[2], (SEQ, D), 1.0, 6.0, ((0, 8), (1, 4))),
        "grad_out": gaussian(arg_keys[3], (SEQ, D), 1.0, 6.0, ((0, 8), (1, 4))),
        "short_filters": gaussian(arg_keys[4], (3, TAPS, D), TAPS ** -0.5, 3.5, ((2, 4),), jnp.float32),
        "long_filter": gaussian(arg_keys[5], (FILT, D), FILT ** -0.5, 0.5, ((1, 4),), jnp.float32),
        "skip_gain": jnp.clip(0.5 + 1.0 * jax.random.uniform(arg_keys[6], (D,), jnp.float32) ** levels(arg_keys[6], (D,), ((0, 4),), -0.2, 0.2), 0.5, 1.5),
    }


def one_block(packed):
    query_in, key_in, value_in, upstream, taps_w, filt, gain = packed
    length = query_in.shape[0]
    ntap = taps_w.shape[1]

    def short_conv(signal, weights):
        padded = jnp.pad(signal, ((ntap - 1, 0), (0, 0)))
        total = jnp.zeros_like(signal)
        for index in range(ntap):
            total = total + weights[index] * padded[ntap - 1 - index:ntap - 1 - index + length]
        return total

    def short_back(grad, weights, signal):
        grad_pad = jnp.pad(grad, ((0, ntap - 1), (0, 0)))
        sig_pad = jnp.pad(signal, ((ntap - 1, 0), (0, 0)))
        result = jnp.zeros_like(grad)
        rows_taps = []
        for index in range(ntap):
            result = result + weights[index] * grad_pad[index:index + length]
            rows_taps.append(jnp.sum(grad * sig_pad[ntap - 1 - index:ntap - 1 - index + length], axis=0))
        return result, jnp.stack(rows_taps)

    q_sig = query_in.astype(jnp.float32)
    k_sig = key_in.astype(jnp.float32)
    v_sig = value_in.astype(jnp.float32)
    dy_sig = upstream.astype(jnp.float32)
    q_feat = short_conv(q_sig, taps_w[0])
    k_feat = short_conv(k_sig, taps_w[1])
    v_feat = short_conv(v_sig, taps_w[2])
    z_feat = k_feat * v_feat
    double = 2 * length
    spec_h = jnp.fft.rfft(filt, n=double, axis=0)
    spec_z = jnp.fft.rfft(z_feat, n=double, axis=0)
    s_feat = jnp.fft.irfft(spec_z * spec_h, n=double, axis=0)[:length].astype(jnp.float32) + gain * z_feat
    grad_q = dy_sig * s_feat
    grad_s = dy_sig * q_feat
    spec_s = jnp.fft.rfft(grad_s, n=double, axis=0)
    grad_z = jnp.fft.irfft(spec_s * jnp.conj(spec_h), n=double, axis=0)[:length].astype(jnp.float32) + gain * grad_s
    grad_k = grad_z * v_feat
    grad_v = grad_z * k_feat
    grad_filt = jnp.fft.irfft(spec_s * jnp.conj(spec_z), n=double, axis=0)[:filt.shape[0]].astype(jnp.float32)
    grad_gain = jnp.sum(grad_s * z_feat, axis=0)
    back_q, taps_q = short_back(grad_q, taps_w[0], q_sig)
    back_k, taps_k = short_back(grad_k, taps_w[1], k_sig)
    back_v, taps_v = short_back(grad_v, taps_w[2], v_sig)
    return (back_q.astype(jnp.bfloat16), back_k.astype(jnp.bfloat16), back_v.astype(jnp.bfloat16),
            grad_filt, jnp.stack([taps_q, taps_k, taps_v]), grad_gain)


def reference(input_q, input_k, input_v, grad_out, short_filters, long_filter, skip_gain):
    length, width = input_q.shape
    block = math.gcd(width, 512)
    count = width // block

    def split(array):
        return array.reshape(array.shape[0], count, block).transpose(1, 0, 2)

    def merge(array):
        return array.transpose(1, 0, 2).reshape(array.shape[1], width)

    packed = (split(input_q), split(input_k), split(input_v), split(grad_out),
              short_filters.reshape(3, short_filters.shape[1], count, block).transpose(2, 0, 1, 3),
              split(long_filter), skip_gain.reshape(count, block))
    back_q, back_k, back_v, grad_filt, grad_taps, grad_gain = lax.map(one_block, packed)
    grad_taps = grad_taps.transpose(1, 2, 0, 3).reshape(3, short_filters.shape[1], width)
    return (merge(back_q), merge(back_k), merge(back_v), merge(grad_filt), grad_taps, grad_gain.reshape(width))
```

```python
import functools

import jax
import jax.numpy as jnp
import numpy as np
from jax import lax
from jax.experimental import pallas as pl
from jax.experimental.pallas import tpu as pltpu
from jax.sharding import PartitionSpec as P

F32 = jnp.float32
BF16 = jnp.bfloat16
ROWS = 16
VMEM_MIB = 52
UNROLL = 2


def transforms(span):
    freq = np.concatenate([np.arange(0, span, 2), np.arange(1, span, 2)]) + 0.5
    angle = np.pi * np.outer(freq, np.arange(span)) / span
    fwd = np.concatenate([np.cos(angle), -np.sin(angle)], 0)
    inv = fwd.T / span

    def halves(mat):
        mat = mat.astype(np.float32)
        high = mat.astype(jnp.bfloat16)
        low = (mat - high.astype(np.float32)).astype(jnp.bfloat16)
        return high, low

    fh, fl = halves(fwd)
    ih, il = halves(inv)
    return (
        np.concatenate([np.concatenate([fh, fh], 1), np.concatenate([fl, fl], 1)], 0),
        np.concatenate([ih, il], 0),
        np.concatenate([np.eye(span)[::-1]] * 2, 1).astype(jnp.bfloat16),
    )


def split(value):
    high = value.astype(BF16)
    low = (value - high.astype(F32)).astype(BF16)
    return high, low


def remote(src, dst, send, recv, target):
    return pltpu.make_async_remote_copy(
        src_ref=src,
        dst_ref=dst,
        send_sem=send,
        recv_sem=recv,
        device_id={"seq": target},
        device_id_type=pl.DeviceIdType.MESH,
    )


def kernel(
    size, length, span, ntap, pad,
    q_all, k_all, v_all, g_all, sf_hbm, lf_hbm, gain_hbm, fh_hbm, ih_hbm, flip_hbm,
    bq_ref, bk_ref, bv_ref, filt_ref, taps_ref, skip_ref,
    q_in, k_in, v_in, g_in, lf_in, sf_ref, gain_in, fh_ref, ih_ref, flip_ref,
    kx, vx, qx, gx, kf, vf, zf, gs, zh, zl, gh, gl, zw, gw, hw, sx, gz, prod, acc, part, gqs, gks, gvs, sums,
    kp_all, vp_all, qp_all, qn_all, gn_all, kn_all, vn_all,
    mine, theirs, chip, others, smine, stheirs, schip, sothers, half, other_half,
    load_sem, fix_sem, halo_send, halo_recv,
    pair_send, pair_recv, chip_send, chip_recv,
    spair_send, spair_recv, schip_send, schip_recv, last_send, last_recv,
):
    _, ncol, _, lane = zh.shape
    width = ncol * lane
    hlf = width // 2
    half_span = span // 2
    nblk = length // span
    big = span + pad
    tile = pl.program_id(0)
    tiles = kp_all.shape[0]
    chips = size // 2
    block = span // size
    me = lax.axis_index("seq")
    core = lax.rem(me, 2)
    place = me // 2
    partner = me + 1 - 2 * core

    def cols_of(t):
        return pl.ds(pl.multiple_of(t * width, width), width)

    def to_next(t):
        cols = cols_of(t)
        target = lax.rem(me + 1, size)
        parts = ((k_all, big, kp_all), (v_all, big, vp_all), (q_all, pad, qp_all))
        return [
            remote(src.at[pl.ds(length - rows, rows), cols], dst.at[t], halo_send.at[t, j], halo_recv.at[t, j], target)
            for j, (src, rows, dst) in enumerate(parts)
        ]

    def to_prev(t):
        cols = cols_of(t)
        target = lax.rem(me + size - 1, size)
        parts = ((q_all, big, qn_all), (g_all, big, gn_all), (k_all, pad, kn_all), (v_all, pad, vn_all))
        return [
            remote(src.at[pl.ds(0, rows), cols], dst.at[t], halo_send.at[t, 3 + j], halo_recv.at[t, 3 + j], target)
            for j, (src, rows, dst) in enumerate(parts)
        ]

    def pair_copy(t):
        return remote(mine.at[t, 1 - core], theirs.at[t], pair_send.at[t], pair_recv.at[t], partner)

    def chip_copy(t, d):
        there = lax.rem(place + d, chips)
        return remote(chip.at[t, there], others.at[t, d], chip_send.at[t, d], chip_recv.at[t, d], there * 2 + core)

    def spair_copy(t):
        return remote(smine.at[t, 1 - core], stheirs.at[t], spair_send.at[t], spair_recv.at[t], partner)

    def schip_copy(t, d):
        there = lax.rem(place + d, chips)
        return remote(schip.at[t], sothers.at[t, d], schip_send.at[t, d], schip_recv.at[t, d], there * 2 + core)

    def last_copy():
        return remote(half, other_half, last_send, last_recv, partner)

    def loads(t):
        cols = cols_of(t)
        pairs = ((k_all, k_in), (v_all, v_in), (q_all, q_in), (g_all, g_in))
        out = [pltpu.make_async_copy(lf_hbm.at[:, cols], lf_in.at[:, cols], load_sem.at[t, 0])]
        for j, (a, b) in enumerate(pairs):
            for c in range(ncol):
                strip = pl.ds(pl.multiple_of(t * width + c * lane, lane), lane)
                out.append(pltpu.make_async_copy(a.at[:, strip], b.at[t * ncol + c], load_sem.at[t, 1 + j * ncol + c]))
        return out

    def fixed():
        pairs = ((sf_hbm, sf_ref), (fh_hbm, fh_ref), (ih_hbm, ih_ref), (flip_hbm, flip_ref), (gain_hbm, gain_in))
        return [pltpu.make_async_copy(a, b, fix_sem.at[j]) for j, (a, b) in enumerate(pairs)]

    @pl.when(tile == 0)
    def _():
        barrier = pltpu.get_barrier_semaphore()
        for d in range(1, size):
            pl.semaphore_signal(
                barrier, inc=1, device_id={"seq": lax.rem(me + d, size)}, device_id_type=pl.DeviceIdType.MESH
            )
        for copy in loads(0) + fixed():
            copy.start()
        pl.semaphore_wait(barrier, size - 1)

        def send(t, _):
            @pl.when(me < size - 1)
            def _():
                for copy in to_next(t):
                    copy.start()

            @pl.when(me > 0)
            def _():
                for copy in to_prev(t):
                    copy.start()

            return 0

        lax.fori_loop(0, tiles, send, 0)

        def fetch(t, _):
            for copy in loads(t):
                copy.start()
            return 0

        lax.fori_loop(1, tiles, fetch, 0)

        @pl.when(me == 0)
        def _():
            for ref in (kp_all, vp_all, qp_all):
                ref[...] = jnp.zeros_like(ref)

        @pl.when(me == size - 1)
        def _():
            for ref in (qn_all, gn_all, kn_all, vn_all):
                ref[...] = jnp.zeros_like(ref)

        for copy in fixed():
            copy.wait()

    kp_ref, vp_ref, qp_ref = kp_all.at[tile], vp_all.at[tile], qp_all.at[tile]
    qn_ref, gn_ref, kn_ref, vn_ref = qn_all.at[tile], gn_all.at[tile], kn_all.at[tile], vn_all.at[tile]

    def join_long(t):
        pair_copy(t).wait_recv()
        chip[t] = mine[t, core] + theirs[t]
        others[t, 0] = mine[t, core, place] + theirs[t, place]
        for d in range(1, chips):
            chip_copy(t, d).start()

    def join_small(t):
        spair_copy(t).wait_recv()
        total = smine[t, core] + stheirs[t]
        schip[t] = total
        sothers[t, 0] = total
        for d in range(1, chips):
            schip_copy(t, d).start()

    for copy in loads(tile):
        copy.wait()

    def here(c):
        return pl.ds(pl.multiple_of(tile * width + c * lane, lane), lane)

    def cut(c):
        return slice(c * lane, (c + 1) * lane)

    def taps(which, c):
        return [jnp.broadcast_to(sf_ref[which, i : i + 1, here(c)], (ROWS, lane)) for i in range(ntap)]

    weights = [[taps(w, c) for c in range(ncol)] for w in range(3)]

    def conv(ref, c, row, first, w):
        total = w[c][0] * first
        for i in range(1, ntap):
            total = total + w[c][i] * ref[c, pl.ds(row - i, ROWS), :]
        return total

    def slot(b):
        return 0 if b == 0 else 3 if b < 0 or b == nblk else 1 + b % 2

    def put(high, low, row, c, value):
        h, l = split(value)
        at = slot(row // span), c, pl.ds(row % span, ROWS)
        high[at] = h
        low[at] = l

    def make_z(row, c, a0, b0, keep_taps, keep_z, keep_split=True):
        a = conv(kx, c, row + big, a0, weights[1])
        b = conv(vx, c, row + big, b0, weights[2])
        z = a * b
        if keep_taps:
            kf[c, pl.ds(row, ROWS), :] = a
            vf[c, pl.ds(row, ROWS), :] = b
        if keep_z:
            zf[c, pl.ds(row - (length - span), ROWS), :] = z
        if keep_split:
            put(zh, zl, row, c, z)

    def make_g(row, c, q0, g0, keep_g, keep_split=True):
        g = g0 * conv(qx, c, row + pad, q0, weights[0])
        if keep_g:
            gs[c, pl.ds(row - length, ROWS), :] = g
        if keep_split:
            put(gh, gl, row, c, g)

    def own(row, c, keep_z):
        a0 = k_in[tile * ncol + c, pl.ds(row, ROWS), :].astype(F32)
        b0 = v_in[tile * ncol + c, pl.ds(row, ROWS), :].astype(F32)
        q0 = q_in[tile * ncol + c, pl.ds(row, ROWS), :].astype(F32)
        g0 = g_in[tile * ncol + c, pl.ds(row, ROWS), :].astype(F32)
        kx[c, pl.ds(row + big, ROWS), :] = a0
        vx[c, pl.ds(row + big, ROWS), :] = b0
        qx[c, pl.ds(row + pad, ROWS), :] = q0
        gx[c, pl.ds(row, ROWS), :] = g0
        make_z(row, c, a0, b0, True, keep_z)
        make_g(row, c, q0, g0, False)

    def wide(strips):
        return jnp.concatenate(list(strips), 1)

    def spectrum(high, low):
        both = jnp.dot(fh_ref[...], jnp.concatenate([high, low], 0), preferred_element_type=F32)
        return both[: 2 * span] + both[2 * span :]

    def forward(high, low, b, out):
        at = slot(b)
        out[...] = spectrum(wide(high[at, c] for c in range(ncol)), wide(low[at, c] for c in range(ncol)))

    gain = gain_in[:, cols_of(tile)]
    taps_h = lf_in[:, cols_of(tile)]
    first = lax.broadcasted_iota(jnp.int32, (span, width), 0) == 0
    hh, hl = split(taps_h + jnp.where(first, gain, 0.0))
    hw[...] = spectrum(hh, hl)
    for c in range(ncol):
        a0 = k_in[tile * ncol + c, :ROWS, :].astype(F32)
        b0 = v_in[tile * ncol + c, :ROWS, :].astype(F32)
        q0 = q_in[tile * ncol + c, :ROWS, :].astype(F32)
        kx[c, big : big + ROWS, :] = a0
        vx[c, big : big + ROWS, :] = b0
        qx[c, pad : pad + ROWS, :] = q0
        gx[c, :ROWS, :] = g_in[tile * ncol + c, :ROWS, :].astype(F32)
    def own_block(b):
        for c in range(ncol):
            for r in range(span // ROWS):
                if b + r > 0:
                    own(b * span + r * ROWS, c, b == nblk - 1)

    early = nblk // 2
    for b in range(early):
        own_block(b)

    @pl.when(me > 0)
    def _():
        for copy in to_next(tile):
            copy.wait_recv()

    @pl.when(me < size - 1)
    def _():
        for copy in to_prev(tile):
            copy.wait_recv()

    for c in range(ncol):
        for ref, src, at in (
            (kx, kp_ref, 0), (vx, vp_ref, 0), (qx, qp_ref, 0),
            (kx, kn_ref, big + length), (vx, vn_ref, big + length), (qx, qn_ref, pad + length),
            (gx, gn_ref, length),
        ):
            ref[c, at : at + src.shape[0], :] = src[:, cut(c)].astype(F32)

    def rows_of(ref, c, row):
        return ref[c, row : row + ROWS, :]

    for c in range(ncol):
        make_z(0, c, rows_of(kx, c, big), rows_of(vx, c, big), True, False)
        make_g(0, c, rows_of(qx, c, pad), rows_of(gx, c, 0), False)
    for b in range(1, early):
        forward(zh, zl, b, zw.at[b + 1])
        forward(gh, gl, b, gw.at[b])
    forward(zh, zl, 0, zw.at[1])
    forward(gh, gl, 0, gw.at[0])
    for b in range(early, nblk):
        own_block(b)
        forward(zh, zl, b, zw.at[b + 1])
        forward(gh, gl, b, gw.at[b])
    for c in range(ncol):
        for r in range(span // ROWS):
            row = r * ROWS - span
            make_z(row, c, rows_of(kx, c, row + big), rows_of(vx, c, row + big), False, False)
    forward(zh, zl, -1, zw.at[0])
    for c in range(ncol):
        for r in range(span // ROWS + 1):
            row = length + r * ROWS
            make_g(row, c, rows_of(qx, c, row + pad), rows_of(gx, c, row), True, r < span // ROWS)
        row = length
        make_z(row, c, rows_of(kx, c, row + big), rows_of(vx, c, row + big), True, True, False)
    forward(gh, gl, nblk, gw.at[nblk])
    back_h = jnp.dot(flip_ref[...], jnp.concatenate(split(taps_h), 0), preferred_element_type=F32)
    line = lax.broadcasted_iota(jnp.int32, (8, lane), 0)
    for c in range(ncol):
        edge_s = jnp.zeros((8, lane), F32)
        edge_z = jnp.zeros((8, lane), F32)
        for i in range(ntap - 1):
            zrow = zf[c, span + i : span + i + 1, :]
            grow = gs[c, i : i + 1, :]
            win = zf[c, i + 1 : i + 1 + span, :]
            value = jnp.sum(win * back_h[:, cut(c)], axis=0, keepdims=True) + gain[:, cut(c)] * zrow
            edge_s = jnp.where(line == i, value, edge_s)
            win = gs[c, i : i + span, :]
            value = jnp.sum(win * taps_h[:, cut(c)], axis=0, keepdims=True) + gain[:, cut(c)] * grow
            edge_z = jnp.where(line == i, value, edge_z)
        gqs[c, length : length + 8, :] = gx[c, length : length + 8, :] * edge_s
        gks[c, length : length + 8, :] = edge_z * vf[c, length : length + 8, :]
        gvs[c, length : length + 8, :] = edge_z * kf[c, length : length + 8, :]

    steps = span // ROWS * ncol

    def product(blocks, sign, n, _):
        if isinstance(n, int):
            re, im = pl.ds(n // ncol * ROWS, ROWS), pl.ds(n // ncol * ROWS + span, ROWS)
            pc = n % ncol
            col = cut(pc)
        else:
            fr = pl.multiple_of(n // ncol * ROWS, ROWS)
            re, im = pl.ds(fr, ROWS), pl.ds(fr + span, ROWS)
            pc = lax.rem(n, ncol)
            col = pl.ds(pl.multiple_of(pc * lane, lane), lane)

        def store(at, rows, value):
            h, l = split(value)
            prod[at, 0, pc, rows, :] = h
            prod[at, 1, pc, rows, :] = l

        hr, hi = hw[re, col], hw[im, col]
        b = blocks[0]
        zr, zi = zw[b, re, col], zw[b, im, col]
        gr, gi = gw[b, re, col], gw[b, im, col]
        ar = ai = None
        if b == 0:
            ar, ai = acc[re, col], acc[im, col]
        for b in blocks:
            zr2, zi2 = zw[b + 1, re, col], zw[b + 1, im, col]
            gr2, gi2 = gw[b + 1, re, col], gw[b + 1, im, col]
            if sign > 0:
                yr, yi = zr2 - zi, zi2 + zr
                xr, xi = gr + gi2, gi - gr2
            else:
                yr, yi = zr2 + zi, zi2 - zr
                xr, xi = gr - gi2, gi + gr2
            store(2 * b, re, yr * hr - yi * hi)
            store(2 * b, im, yr * hi + yi * hr)
            store(2 * b + 1, re, xr * hr + xi * hi)
            store(2 * b + 1, im, xi * hr - xr * hi)
            tr, ti = gr * yr + gi * yi, gi * yr - gr * yi
            ar, ai = (tr, ti) if ar is None else (ar + tr, ai + ti)
            zr, zi, gr, gi = zr2, zi2, gr2, gi2
        if blocks[0] == 0:
            store(2 * nblk, re, ar)
            store(2 * nblk, im, ai)
        else:
            acc[re, col] = ar
            acc[im, col] = ai
        return 0

    @pl.when(tile > 0)
    def _():
        join_long(tile - 1)
        join_small(tile - 1)

    late = range(nblk // 2, nblk)
    lax.fori_loop(0, steps // 2, functools.partial(product, late, 1), 0, unroll=UNROLL)
    lax.fori_loop(steps // 2, steps, functools.partial(product, late, -1), 0, unroll=UNROLL)

    def inverse(at, out):
        both = jnp.dot(ih_ref[...], wide(prod[at, 0, c] for c in range(ncol)), preferred_element_type=F32)
        rest = jnp.dot(ih_ref[:span], wide(prod[at, 1, c] for c in range(ncol)), preferred_element_type=F32)
        out[...] = both[:span] + both[span:] + rest


    def back_to_time(b):
        inverse(2 * b, sx.at[b % 2])
        inverse(2 * b + 1, gz.at[b % 2])

    back_to_time(nblk - 1)
    for n in range(steps):
        product(range(nblk // 2), 1 if n < steps // 2 else -1, n, 0)
    inverse(2 * nblk, part)
    for d in range(size):
        mine[tile, d % 2, d // 2] = part[d * block : (d + 1) * block]
    pair_copy(tile).start()

    def fold(value):
        total = value[:8]
        for r in range(8, ROWS, 8):
            total = total + value[r : r + 8]
        return total

    per = span // ROWS
    sums[...] = jnp.zeros_like(sums)

    def last(b):
        if b > 0:
            back_to_time(b - 1)
        for c in range(ncol):
            total = [[sums[w, i, :, cut(c)] for i in range(ntap)] for w in range(3)]
            for r in range(per):
                row = b * span + (per - 1 - r) * ROWS
                at = pl.ds(row, ROWS)
                inner = slice(row - b * span, row - b * span + ROWS)
                gzc = gz[b % 2, inner, cut(c)]
                grads = (gx[c, at, :] * sx[b % 2, inner, cut(c)], gzc * vf[c, at, :], gzc * kf[c, at, :])
                for w, (grad, ref, own_x, off, out) in enumerate(zip(
                    grads, (gqs, gks, gvs), (qx, kx, vx), (pad, big, big), (bq_ref, bk_ref, bv_ref)
                )):
                    ref[c, at, :] = grad
                    x = own_x[c, pl.ds(row + off, ROWS), :]
                    res = weights[w][c][0] * grad
                    total[w][0] = total[w][0] + fold(grad * x)
                    for i in range(1, ntap):
                        later = ref[c, pl.ds(row + i, ROWS), :]
                        res = res + weights[w][c][i] * later
                        total[w][i] = total[w][i] + fold(later * x)
                    out[tile * ncol + c, at, :] = res.astype(BF16)
            for w in range(3):
                for i in range(ntap):
                    sums[w, i, :, cut(c)] = total[w][i]

    for b in reversed(range(nblk)):
        last(b)
    rows = [jnp.sum(sums[w, i], axis=0, keepdims=True) for w in range(3) for i in range(ntap)]
    rows.append(part[0:1, :])
    small = jnp.concatenate(rows + [jnp.zeros((pad - len(rows), width), F32)], 0)
    for p in range(2):
        smine[tile, p] = small[:, p * hlf : (p + 1) * hlf]
    spair_copy(tile).start()

    @pl.when(tile == tiles - 1)
    def _():
        join_long(tiles - 1)
        join_small(tiles - 1)

        def finish(t, _):
            cols = cols_of(t)

            @pl.when(me < size - 1)
            def _():
                for copy in to_next(t):
                    copy.wait_send()

            @pl.when(me > 0)
            def _():
                for copy in to_prev(t):
                    copy.wait_send()

            pair_copy(t).wait_send()
            spair_copy(t).wait_send()
            for d in range(1, chips):
                chip_copy(t, d).wait_send()
                chip_copy(t, d).wait_recv()
                schip_copy(t, d).wait_send()
                schip_copy(t, d).wait_recv()
            total = others[t, place]
            small = sothers[t, place]
            for z in range(1, chips):
                d = lax.rem(place + chips - z, chips)
                total = total + others[t, d]
                small = small + sothers[t, d]
            filt_ref[:, cols] = total
            half[t] = small
            return 0

        lax.fori_loop(0, tiles, finish, 0)
        last_copy().start()
        last_copy().wait()

        def write(t, _):
            for p in range(2):
                own_half = half[t]
                total = jnp.where(core == p, own_half, other_half[t])
                cols = pl.ds(pl.multiple_of(t * width + p * hlf, hlf), hlf)
                for w in range(3):
                    for i in range(ntap):
                        at = w * ntap + i
                        taps_ref[w, i : i + 1, cols] = total[at : at + 1]
                skip_ref[:, cols] = total[3 * ntap : 3 * ntap + 1]
            return 0

        lax.fori_loop(0, tiles, write, 0)


def settle(*refs):
    half = len(refs) // 2
    sem = refs[-1]
    copies = []
    for src, dst in zip(refs[:half], refs[half:-1]):
        if src.shape == dst.shape:
            copies.append((src, dst))
        else:
            lane = src.shape[2]
            copies += [(src.at[n], dst.at[:, n * lane : (n + 1) * lane]) for n in range(src.shape[0])]
    copies = [pltpu.make_async_copy(src, dst, sem.at[n]) for n, (src, dst) in enumerate(copies)]
    for copy in copies:
        copy.start()
    for copy in copies:
        copy.wait()


def body(input_q, input_k, input_v, grad_out, short_filters, long_filter, skip_gain):
    length, channels = input_q.shape
    ntap = short_filters.shape[1]
    span = long_filter.shape[0]
    pad = 16
    lane = 128
    big = span + pad
    width = min(256, channels)
    mats = [jnp.asarray(m) for m in transforms(span)]
    nblk = length // span

    size = lax.axis_size("seq")
    tiles = channels // width
    chips = size // 2
    block = span // size
    ncol = width // lane
    cells = lambda *rows: pltpu.VMEM((*rows, width), F32)
    strips = lambda rows: pltpu.VMEM((ncol, rows, lane), F32)
    halves = lambda *rows: pltpu.VMEM((*rows, lane), BF16)
    edge = lambda rows: pltpu.VMEM((tiles, rows, width), BF16)
    small = lambda *lead: pltpu.VMEM((*lead, pad, width // 2), F32)
    dma = lambda *shape: pltpu.SemaphoreType.DMA(shape)
    whole = pl.BlockSpec(memory_space=pltpu.VMEM)
    outs = pl.pallas_call(
        functools.partial(kernel, size, length, span, ntap, pad),
        grid=(tiles,),
        out_shape=(
            *[pltpu.VMEM((tiles * ncol, length, lane), BF16) for _ in range(3)],
            pltpu.VMEM((block, channels), F32),
            pltpu.VMEM((3, ntap, channels), F32),
            pltpu.VMEM((1, channels), F32),
        ),
        in_specs=[pl.BlockSpec(memory_space=pltpu.HBM)] * 10,
        out_specs=(whole,) * 6,
        scratch_shapes=[
            *[pltpu.VMEM((tiles * ncol, length, lane), BF16) for _ in range(4)],
            pltpu.VMEM((span, channels), F32), pltpu.VMEM((3, ntap, channels), F32), pltpu.VMEM((1, channels), F32),
            *[pltpu.VMEM(m.shape, BF16) for m in mats],
            strips(length + big + pad), strips(length + big + pad), strips(length + big + pad), strips(length + big),
            strips(length + pad), strips(length + pad), strips(span + pad), strips(span + pad),
            *[halves(4, ncol, span) for _ in range(4)],
            cells(nblk + 1, 2 * span), cells(nblk + 1, 2 * span), cells(2 * span), cells(2, span), cells(2, span),
            halves(2 * nblk + 1, 2, ncol, 2 * span), cells(2 * span), cells(span),
            strips(length + pad), strips(length + pad), strips(length + pad), cells(3, ntap, 8),
            edge(big), edge(big), edge(pad), edge(big), edge(big), edge(pad), edge(pad),
            cells(tiles, 2, chips, block), cells(tiles, chips, block),
            cells(tiles, chips, block), cells(tiles, chips, block),
            small(tiles, 2), small(tiles), small(tiles), small(tiles, chips), small(tiles), small(tiles),
            dma(tiles, 1 + 4 * ncol), dma(5), dma(tiles, 7), dma(tiles, 7),
            dma(tiles), dma(tiles), dma(tiles, chips), dma(tiles, chips),
            dma(tiles), dma(tiles), dma(tiles, chips), dma(tiles, chips),
            pltpu.SemaphoreType.DMA, pltpu.SemaphoreType.DMA,
        ],
        compiler_params=pltpu.CompilerParams(
            dimension_semantics=("arbitrary",),
            vmem_limit_bytes=VMEM_MIB * 1024 * 1024,
            collective_id=0,
            has_side_effects=True,
        ),
        name="hyena_back",
    )(input_q, input_k, input_v, grad_out, short_filters, long_filter, skip_gain[None], *mats)
    outs = [pltpu.with_memory_space_constraint(out, pltpu.VMEM) for out in outs]
    back_q, back_k, back_v, grad_filt, grad_taps, grad_gain = pl.pallas_call(
        settle,
        out_shape=tuple(
            jax.ShapeDtypeStruct((length, channels) if n < 3 else out.shape, out.dtype) for n, out in enumerate(outs)
        ),
        in_specs=[whole] * 6,
        out_specs=(pl.BlockSpec(memory_space=pltpu.HBM),) * 6,
        scratch_shapes=[dma(3 * tiles * ncol + 3)],
        compiler_params=pltpu.CompilerParams(vmem_limit_bytes=1024 * 1024),
        name="settle",
    )(*outs)
    return (back_q, back_k, back_v, grad_filt, grad_taps, grad_gain[0])


def solution(mesh):
    return jax.shard_map(
        body,
        mesh=mesh,
        in_specs=(
            P("seq", "ch"),
            P("seq", "ch"),
            P("seq", "ch"),
            P("seq", "ch"),
            P(None, None, "ch"),
            P(None, "ch"),
            P("ch"),
        ),
        out_specs=(
            P("seq", "ch"),
            P("seq", "ch"),
            P("seq", "ch"),
            P("seq", "ch"),
            P(None, None, "ch"),
            P("ch"),
        ),
        check_vma=False,
    )
```

```python
import functools

import jax
import jax.numpy as jnp
import numpy as np
from jax import lax
from jax.experimental import pallas as pl
from jax.experimental.pallas import tpu as pltpu
from jax.sharding import PartitionSpec as P

F32 = jnp.float32
BF16 = jnp.bfloat16
ROWS = 16
VMEM_MIB = 52
UNROLL = 2


def transforms(span):
    freq = np.concatenate([np.arange(0, span, 2), np.arange(1, span, 2)]) + 0.5
    angle = np.pi * np.outer(freq, np.arange(span)) / span
    fwd = np.concatenate([np.cos(angle), -np.sin(angle)], 0)
    inv = fwd.T / span

    def halves(mat):
        mat = mat.astype(np.float32)
        high = mat.astype(jnp.bfloat16)
        low = (mat - high.astype(np.float32)).astype(jnp.bfloat16)
        return high, low

    fh, fl = halves(fwd)
    ih, il = halves(inv)
    return (
        np.concatenate([np.concatenate([fh, fh], 1), np.concatenate([fl, fl], 1)], 0),
        np.concatenate([ih, il], 0),
        np.concatenate([np.eye(span)[::-1]] * 2, 1).astype(jnp.bfloat16),
    )


def split(value):
    high = value.astype(BF16)
    low = (value - high.astype(F32)).astype(BF16)
    return high, low


def remote(src, dst, send, recv, target):
    return pltpu.make_async_remote_copy(
        src_ref=src,
        dst_ref=dst,
        send_sem=send,
        recv_sem=recv,
        device_id={"seq": target},
        device_id_type=pl.DeviceIdType.MESH,
    )


def kernel(
    size, length, span, ntap, pad,
    q_all, k_all, v_all, g_all, sf_hbm, lf_hbm, gain_hbm, fh_hbm, ih_hbm, flip_hbm,
    bq_ref, bk_ref, bv_ref, filt_ref, taps_ref, skip_ref,
    q_in, k_in, v_in, g_in, lf_in, sf_ref, gain_in, fh_ref, ih_ref, flip_ref,
    kx, vx, qx, gx, kf, vf, zf, gs, zh, zl, gh, gl, zw, gw, hw, sx, gz, prod, acc, part, gqs, gks, gvs, sums,
    kp_all, vp_all, qp_all, qn_all, gn_all, kn_all, vn_all,
    mine, theirs, chip, others, smine, stheirs, schip, sothers, half, other_half,
    load_sem, fix_sem, halo_send, halo_recv,
    pair_send, pair_recv, chip_send, chip_recv,
    spair_send, spair_recv, schip_send, schip_recv, last_send, last_recv,
):
    _, ncol, _, lane = zh.shape
    width = ncol * lane
    hlf = width // 2
    half_span = span // 2
    nblk = length // span
    big = span + pad
    tile = pl.program_id(0)
    tiles = kp_all.shape[0]
    chips = size // 2
    block = span // size
    me = lax.axis_index("seq")
    core = lax.rem(me, 2)
    place = me // 2
    partner = me + 1 - 2 * core

    def cols_of(t):
        return pl.ds(pl.multiple_of(t * width, width), width)

    def to_next(t):
        cols = cols_of(t)
        target = lax.rem(me + 1, size)
        parts = ((k_all, big, kp_all), (v_all, big, vp_all), (q_all, pad, qp_all))
        return [
            remote(src.at[pl.ds(length - rows, rows), cols], dst.at[t], halo_send.at[t, j], halo_recv.at[t, j], target)
            for j, (src, rows, dst) in enumerate(parts)
        ]

    def to_prev(t):
        cols = cols_of(t)
        target = lax.rem(me + size - 1, size)
        parts = ((q_all, big, qn_all), (g_all, big, gn_all), (k_all, pad, kn_all), (v_all, pad, vn_all))
        return [
            remote(src.at[pl.ds(0, rows), cols], dst.at[t], halo_send.at[t, 3 + j], halo_recv.at[t, 3 + j], target)
            for j, (src, rows, dst) in enumerate(parts)
        ]

    def pair_copy(t):
        return remote(mine.at[t, 1 - core], theirs.at[t], pair_send.at[t], pair_recv.at[t], partner)

    def chip_copy(t, d):
        there = lax.rem(place + d, chips)
        return remote(chip.at[t, there], others.at[t, d], chip_send.at[t, d], chip_recv.at[t, d], there * 2 + core)

    def spair_copy(t):
        return remote(smine.at[t, 1 - core], stheirs.at[t], spair_send.at[t], spair_recv.at[t], partner)

    def schip_copy(t, d):
        there = lax.rem(place + d, chips)
        return remote(schip.at[t], sothers.at[t, d], schip_send.at[t, d], schip_recv.at[t, d], there * 2 + core)

    def last_copy():
        return remote(half, other_half, last_send, last_recv, partner)

    def loads(t):
        cols = cols_of(t)
        pairs = ((k_all, k_in), (v_all, v_in), (q_all, q_in), (g_all, g_in))
        out = [pltpu.make_async_copy(lf_hbm.at[:, cols], lf_in.at[:, cols], load_sem.at[t, 0])]
        for j, (a, b) in enumerate(pairs):
            for c in range(ncol):
                strip = pl.ds(pl.multiple_of(t * width + c * lane, lane), lane)
                out.append(pltpu.make_async_copy(a.at[:, strip], b.at[t * ncol + c], load_sem.at[t, 1 + j * ncol + c]))
        return out

    def fixed():
        pairs = ((sf_hbm, sf_ref), (fh_hbm, fh_ref), (ih_hbm, ih_ref), (flip_hbm, flip_ref), (gain_hbm, gain_in))
        return [pltpu.make_async_copy(a, b, fix_sem.at[j]) for j, (a, b) in enumerate(pairs)]

    @pl.when(tile == 0)
    def _():
        barrier = pltpu.get_barrier_semaphore()
        for d in range(1, size):
            pl.semaphore_signal(
                barrier, inc=1, device_id={"seq": lax.rem(me + d, size)}, device_id_type=pl.DeviceIdType.MESH
            )
        for copy in loads(0) + fixed():
            copy.start()
        pl.semaphore_wait(barrier, size - 1)

        def send(t, _):
            @pl.when(me < size - 1)
            def _():
                for copy in to_next(t):
                    copy.start()

            @pl.when(me > 0)
            def _():
                for copy in to_prev(t):
                    copy.start()

            return 0

        lax.fori_loop(0, tiles, send, 0)

        def fetch(t, _):
            for copy in loads(t):
                copy.start()
            return 0

        lax.fori_loop(1, tiles, fetch, 0)

        @pl.when(me == 0)
        def _():
            for ref in (kp_all, vp_all, qp_all):
                ref[...] = jnp.zeros_like(ref)

        @pl.when(me == size - 1)
        def _():
            for ref in (qn_all, gn_all, kn_all, vn_all):
                ref[...] = jnp.zeros_like(ref)

        for copy in fixed():
            copy.wait()

    kp_ref, vp_ref, qp_ref = kp_all.at[tile], vp_all.at[tile], qp_all.at[tile]
    qn_ref, gn_ref, kn_ref, vn_ref = qn_all.at[tile], gn_all.at[tile], kn_all.at[tile], vn_all.at[tile]

    def join_long(t):
        pair_copy(t).wait_recv()
        chip[t] = mine[t, core] + theirs[t]
        others[t, 0] = mine[t, core, place] + theirs[t, place]
        for d in range(1, chips):
            chip_copy(t, d).start()

    def join_small(t):
        spair_copy(t).wait_recv()
        total = smine[t, core] + stheirs[t]
        schip[t] = total
        sothers[t, 0] = total
        for d in range(1, chips):
            schip_copy(t, d).start()

    for copy in loads(tile):
        copy.wait()

    @pl.when(tile > 1)
    def _():
        join_long(tile - 2)
        join_small(tile - 2)

    @pl.when(me > 0)
    def _():
        for copy in to_next(tile):
            copy.wait_recv()

    @pl.when(me < size - 1)
    def _():
        for copy in to_prev(tile):
            copy.wait_recv()

    def here(c):
        return pl.ds(pl.multiple_of(tile * width + c * lane, lane), lane)

    def cut(c):
        return slice(c * lane, (c + 1) * lane)

    def taps(which, c):
        return [jnp.broadcast_to(sf_ref[which, i : i + 1, here(c)], (ROWS, lane)) for i in range(ntap)]

    weights = [[taps(w, c) for c in range(ncol)] for w in range(3)]

    def conv(ref, c, row, first, w):
        total = w[c][0] * first
        for i in range(1, ntap):
            total = total + w[c][i] * ref[c, pl.ds(row - i, ROWS), :]
        return total

    def slot(b):
        return nblk if b < 0 else b

    def put(high, low, row, c, value):
        h, l = split(value)
        at = slot(row // span), c, pl.ds(row % span, ROWS)
        high[at] = h
        low[at] = l

    def make_z(row, c, a0, b0, keep_taps, keep_z, keep_split=True):
        a = conv(kx, c, row + big, a0, weights[1])
        b = conv(vx, c, row + big, b0, weights[2])
        z = a * b
        if keep_taps:
            kf[c, pl.ds(row, ROWS), :] = a
            vf[c, pl.ds(row, ROWS), :] = b
        if keep_z:
            zf[c, pl.ds(row - (length - span), ROWS), :] = z
        if keep_split:
            put(zh, zl, row, c, z)

    def make_g(row, c, q0, g0, keep_g, keep_split=True):
        g = g0 * conv(qx, c, row + pad, q0, weights[0])
        if keep_g:
            gs[c, pl.ds(row - length, ROWS), :] = g
        if keep_split:
            put(gh, gl, row, c, g)

    def own(row, c, keep_z):
        a0 = k_in[tile * ncol + c, pl.ds(row, ROWS), :].astype(F32)
        b0 = v_in[tile * ncol + c, pl.ds(row, ROWS), :].astype(F32)
        q0 = q_in[tile * ncol + c, pl.ds(row, ROWS), :].astype(F32)
        g0 = g_in[tile * ncol + c, pl.ds(row, ROWS), :].astype(F32)
        kx[c, pl.ds(row + big, ROWS), :] = a0
        vx[c, pl.ds(row + big, ROWS), :] = b0
        qx[c, pl.ds(row + pad, ROWS), :] = q0
        gx[c, pl.ds(row, ROWS), :] = g0
        make_z(row, c, a0, b0, True, keep_z)
        make_g(row, c, q0, g0, False)

    def wide(strips):
        return jnp.concatenate(list(strips), 1)

    def spectrum(high, low):
        both = jnp.dot(fh_ref[...], jnp.concatenate([high, low], 0), preferred_element_type=F32)
        return both[: 2 * span] + both[2 * span :]

    def forward(high, low, b, out):
        at = slot(b)
        out[...] = spectrum(wide(high[at, c] for c in range(ncol)), wide(low[at, c] for c in range(ncol)))

    gain = gain_in[:, cols_of(tile)]
    taps_h = lf_in[:, cols_of(tile)]
    first = lax.broadcasted_iota(jnp.int32, (span, width), 0) == 0
    hh, hl = split(taps_h + jnp.where(first, gain, 0.0))
    hw[...] = spectrum(hh, hl)
    for c in range(ncol):
        for ref, src, at in (
            (kx, kp_ref, 0), (vx, vp_ref, 0), (qx, qp_ref, 0),
            (kx, kn_ref, big + length), (vx, vn_ref, big + length), (qx, qn_ref, pad + length),
            (gx, gn_ref, length),
        ):
            ref[c, at : at + src.shape[0], :] = src[:, cut(c)].astype(F32)

    def own_block(b):
        for c in range(ncol):
            for r in range(span // ROWS):
                own(b * span + r * ROWS, c, b == nblk - 1)

    def rows_of(ref, c, row):
        return ref[c, row : row + ROWS, :]

    def forward_z(b):
        forward(zh, zl, b, zw.at[b + 1])

    def forward_g(b):
        forward(gh, gl, b, gw.at[b])

    mid = nblk // 2
    for b in range(nblk):
        own_block(b)
        if b >= mid - 1:
            forward_z(b)
        if b >= mid:
            forward_g(b)
    for c in range(ncol):
        for r in range(span // ROWS + 1):
            row = length + r * ROWS
            make_g(row, c, rows_of(qx, c, row + pad), rows_of(gx, c, row), True, r < span // ROWS)
        row = length
        make_z(row, c, rows_of(kx, c, row + big), rows_of(vx, c, row + big), True, True, False)
    forward_g(nblk)
    for c in range(ncol):
        for r in range(span // ROWS):
            row = r * ROWS - span
            make_z(row, c, rows_of(kx, c, row + big), rows_of(vx, c, row + big), False, False)
    for b in range(mid - 1, -2, -1):
        if b < mid - 1:
            forward_z(b)
        if b >= 0:
            forward_g(b)
    back_h = jnp.dot(flip_ref[...], jnp.concatenate(split(taps_h), 0), preferred_element_type=F32)
    line = lax.broadcasted_iota(jnp.int32, (8, lane), 0)
    for c in range(ncol):
        edge_s = jnp.zeros((8, lane), F32)
        edge_z = jnp.zeros((8, lane), F32)
        for i in range(ntap - 1):
            zrow = zf[c, span + i : span + i + 1, :]
            grow = gs[c, i : i + 1, :]
            win = zf[c, i + 1 : i + 1 + span, :]
            value = jnp.sum(win * back_h[:, cut(c)], axis=0, keepdims=True) + gain[:, cut(c)] * zrow
            edge_s = jnp.where(line == i, value, edge_s)
            win = gs[c, i : i + span, :]
            value = jnp.sum(win * taps_h[:, cut(c)], axis=0, keepdims=True) + gain[:, cut(c)] * grow
            edge_z = jnp.where(line == i, value, edge_z)
        gqs[c, length : length + 8, :] = gx[c, length : length + 8, :] * edge_s
        gks[c, length : length + 8, :] = edge_z * vf[c, length : length + 8, :]
        gvs[c, length : length + 8, :] = edge_z * kf[c, length : length + 8, :]

    steps = span // ROWS * ncol

    def product(blocks, sign, n, _):
        if isinstance(n, int):
            re, im = pl.ds(n // ncol * ROWS, ROWS), pl.ds(n // ncol * ROWS + span, ROWS)
            pc = n % ncol
            col = cut(pc)
        else:
            fr = pl.multiple_of(n // ncol * ROWS, ROWS)
            re, im = pl.ds(fr, ROWS), pl.ds(fr + span, ROWS)
            pc = lax.rem(n, ncol)
            col = pl.ds(pl.multiple_of(pc * lane, lane), lane)

        def store(at, rows, value):
            h, l = split(value)
            prod[at, 0, pc, rows, :] = h
            prod[at, 1, pc, rows, :] = l

        hr, hi = hw[re, col], hw[im, col]
        b = blocks[0]
        zr, zi = zw[b, re, col], zw[b, im, col]
        gr, gi = gw[b, re, col], gw[b, im, col]
        ar = ai = None
        if b == 0:
            ar, ai = acc[re, col], acc[im, col]
        for b in blocks:
            zr2, zi2 = zw[b + 1, re, col], zw[b + 1, im, col]
            gr2, gi2 = gw[b + 1, re, col], gw[b + 1, im, col]
            if sign > 0:
                yr, yi = zr2 - zi, zi2 + zr
                xr, xi = gr + gi2, gi - gr2
            else:
                yr, yi = zr2 + zi, zi2 - zr
                xr, xi = gr - gi2, gi + gr2
            store(2 * b, re, yr * hr - yi * hi)
            store(2 * b, im, yr * hi + yi * hr)
            store(2 * b + 1, re, xr * hr + xi * hi)
            store(2 * b + 1, im, xi * hr - xr * hi)
            tr, ti = gr * yr + gi * yi, gi * yr - gr * yi
            ar, ai = (tr, ti) if ar is None else (ar + tr, ai + ti)
            zr, zi, gr, gi = zr2, zi2, gr2, gi2
        if blocks[0] == 0:
            store(2 * nblk, re, ar)
            store(2 * nblk, im, ai)
        else:
            acc[re, col] = ar
            acc[im, col] = ai
        return 0

    late = range(nblk // 2, nblk)
    for n in range(steps):
        product(late, 1 if n < steps // 2 else -1, n, 0)

    def inverse(at, out):
        both = jnp.dot(ih_ref[...], wide(prod[at, 0, c] for c in range(ncol)), preferred_element_type=F32)
        rest = jnp.dot(ih_ref[:span], wide(prod[at, 1, c] for c in range(ncol)), preferred_element_type=F32)
        out[...] = both[:span] + both[span:] + rest


    def back_to_time(b):
        inverse(2 * b, sx.at[b % 2])
        inverse(2 * b + 1, gz.at[b % 2])

    back_to_time(nblk - 1)
    for n in range(steps):
        product(range(nblk // 2), 1 if n < steps // 2 else -1, n, 0)
    inverse(2 * nblk, part)
    for d in range(size):
        mine[tile, d % 2, d // 2] = part[d * block : (d + 1) * block]
    pair_copy(tile).start()

    def fold(value):
        total = value[:8]
        for r in range(8, ROWS, 8):
            total = total + value[r : r + 8]
        return total

    per = span // ROWS
    sums[...] = jnp.zeros_like(sums)

    def last(b):
        if b > 0:
            back_to_time(b - 1)
        for c in range(ncol):
            total = [[sums[w, i, :, cut(c)] for i in range(ntap)] for w in range(3)]
            for r in range(per):
                row = b * span + (per - 1 - r) * ROWS
                at = pl.ds(row, ROWS)
                inner = slice(row - b * span, row - b * span + ROWS)
                gzc = gz[b % 2, inner, cut(c)]
                grads = (gx[c, at, :] * sx[b % 2, inner, cut(c)], gzc * vf[c, at, :], gzc * kf[c, at, :])
                for w, (grad, ref, own_x, off, out) in enumerate(zip(
                    grads, (gqs, gks, gvs), (qx, kx, vx), (pad, big, big), (bq_ref, bk_ref, bv_ref)
                )):
                    ref[c, at, :] = grad
                    x = own_x[c, pl.ds(row + off, ROWS), :]
                    res = weights[w][c][0] * grad
                    total[w][0] = total[w][0] + fold(grad * x)
                    for i in range(1, ntap):
                        later = ref[c, pl.ds(row + i, ROWS), :]
                        res = res + weights[w][c][i] * later
                        total[w][i] = total[w][i] + fold(later * x)
                    out[tile * ncol + c, at, :] = res.astype(BF16)
            for w in range(3):
                for i in range(ntap):
                    sums[w, i, :, cut(c)] = total[w][i]

    for b in reversed(range(nblk)):
        last(b)
    rows = [jnp.sum(sums[w, i], axis=0, keepdims=True) for w in range(3) for i in range(ntap)]
    rows.append(part[0:1, :])
    small = jnp.concatenate(rows + [jnp.zeros((pad - len(rows), width), F32)], 0)
    for p in range(2):
        smine[tile, p] = small[:, p * hlf : (p + 1) * hlf]
    spair_copy(tile).start()

    @pl.when(tile == tiles - 1)
    def _():
        for t in range(max(tiles - 2, 0), tiles):
            join_long(t)
            join_small(t)

        def finish(t, _):
            cols = cols_of(t)

            @pl.when(me < size - 1)
            def _():
                for copy in to_next(t):
                    copy.wait_send()

            @pl.when(me > 0)
            def _():
                for copy in to_prev(t):
                    copy.wait_send()

            pair_copy(t).wait_send()
            spair_copy(t).wait_send()
            for d in range(1, chips):
                chip_copy(t, d).wait_send()
                chip_copy(t, d).wait_recv()
                schip_copy(t, d).wait_send()
                schip_copy(t, d).wait_recv()
            total = others[t, place]
            small = sothers[t, place]
            for z in range(1, chips):
                d = lax.rem(place + chips - z, chips)
                total = total + others[t, d]
                small = small + sothers[t, d]
            filt_ref[:, cols] = total
            half[t] = small
            return 0

        lax.fori_loop(0, tiles, finish, 0)
        last_copy().start()
        last_copy().wait()

        def write(t, _):
            for p in range(2):
                own_half = half[t]
                total = jnp.where(core == p, own_half, other_half[t])
                cols = pl.ds(pl.multiple_of(t * width + p * hlf, hlf), hlf)
                for w in range(3):
                    for i in range(ntap):
                        at = w * ntap + i
                        taps_ref[w, i : i + 1, cols] = total[at : at + 1]
                skip_ref[:, cols] = total[3 * ntap : 3 * ntap + 1]
            return 0

        lax.fori_loop(0, tiles, write, 0)


def settle(*refs):
    half = len(refs) // 2
    sem = refs[-1]
    copies = []
    for src, dst in zip(refs[:half], refs[half:-1]):
        if src.shape == dst.shape:
            copies.append((src, dst))
        else:
            lane = src.shape[2]
            copies += [(src.at[n], dst.at[:, n * lane : (n + 1) * lane]) for n in range(src.shape[0])]
    copies = [pltpu.make_async_copy(src, dst, sem.at[n]) for n, (src, dst) in enumerate(copies)]
    for copy in copies:
        copy.start()
    for copy in copies:
        copy.wait()


def body(input_q, input_k, input_v, grad_out, short_filters, long_filter, skip_gain):
    length, channels = input_q.shape
    ntap = short_filters.shape[1]
    span = long_filter.shape[0]
    pad = 16
    lane = 128
    big = span + pad
    width = min(256, channels)
    mats = [jnp.asarray(m) for m in transforms(span)]
    nblk = length // span

    size = lax.axis_size("seq")
    tiles = channels // width
    chips = size // 2
    block = span // size
    ncol = width // lane
    cells = lambda *rows: pltpu.VMEM((*rows, width), F32)
    strips = lambda rows: pltpu.VMEM((ncol, rows, lane), F32)
    halves = lambda *rows: pltpu.VMEM((*rows, lane), BF16)
    edge = lambda rows: pltpu.VMEM((tiles, rows, width), BF16)
    small = lambda *lead: pltpu.VMEM((*lead, pad, width // 2), F32)
    dma = lambda *shape: pltpu.SemaphoreType.DMA(shape)
    whole = pl.BlockSpec(memory_space=pltpu.VMEM)
    outs = pl.pallas_call(
        functools.partial(kernel, size, length, span, ntap, pad),
        grid=(tiles,),
        out_shape=(
            *[pltpu.VMEM((tiles * ncol, length, lane), BF16) for _ in range(3)],
            pltpu.VMEM((block, channels), F32),
            pltpu.VMEM((3, ntap, channels), F32),
            pltpu.VMEM((1, channels), F32),
        ),
        in_specs=[pl.BlockSpec(memory_space=pltpu.HBM)] * 10,
        out_specs=(whole,) * 6,
        scratch_shapes=[
            *[pltpu.VMEM((tiles * ncol, length, lane), BF16) for _ in range(4)],
            pltpu.VMEM((span, channels), F32), pltpu.VMEM((3, ntap, channels), F32), pltpu.VMEM((1, channels), F32),
            *[pltpu.VMEM(m.shape, BF16) for m in mats],
            strips(length + big + pad), strips(length + big + pad), strips(length + big + pad), strips(length + big),
            strips(length + pad), strips(length + pad), strips(span + pad), strips(span + pad),
            *[halves(nblk + 1, ncol, span) for _ in range(4)],
            cells(nblk + 1, 2 * span), cells(nblk + 1, 2 * span), cells(2 * span), cells(2, span), cells(2, span),
            halves(2 * nblk + 1, 2, ncol, 2 * span), cells(2 * span), cells(span),
            strips(length + pad), strips(length + pad), strips(length + pad), cells(3, ntap, 8),
            edge(big), edge(big), edge(pad), edge(big), edge(big), edge(pad), edge(pad),
            cells(tiles, 2, chips, block), cells(tiles, chips, block),
            cells(tiles, chips, block), cells(tiles, chips, block),
            small(tiles, 2), small(tiles), small(tiles), small(tiles, chips), small(tiles), small(tiles),
            dma(tiles, 1 + 4 * ncol), dma(5), dma(tiles, 7), dma(tiles, 7),
            dma(tiles), dma(tiles), dma(tiles, chips), dma(tiles, chips),
            dma(tiles), dma(tiles), dma(tiles, chips), dma(tiles, chips),
            pltpu.SemaphoreType.DMA, pltpu.SemaphoreType.DMA,
        ],
        compiler_params=pltpu.CompilerParams(
            dimension_semantics=("arbitrary",),
            vmem_limit_bytes=VMEM_MIB * 1024 * 1024,
            collective_id=0,
            has_side_effects=True,
        ),
        name="hyena_back",
    )(input_q, input_k, input_v, grad_out, short_filters, long_filter, skip_gain[None], *mats)
    outs = [pltpu.with_memory_space_constraint(out, pltpu.VMEM) for out in outs]
    back_q, back_k, back_v, grad_filt, grad_taps, grad_gain = pl.pallas_call(
        settle,
        out_shape=tuple(
            jax.ShapeDtypeStruct((length, channels) if n < 3 else out.shape, out.dtype) for n, out in enumerate(outs)
        ),
        in_specs=[whole] * 6,
        out_specs=(pl.BlockSpec(memory_space=pltpu.HBM),) * 6,
        scratch_shapes=[dma(3 * tiles * ncol + 3)],
        compiler_params=pltpu.CompilerParams(vmem_limit_bytes=1024 * 1024),
        name="settle",
    )(*outs)
    return (back_q, back_k, back_v, grad_filt, grad_taps, grad_gain[0])


def solution(mesh):
    return jax.shard_map(
        body,
        mesh=mesh,
        in_specs=(
            P("seq", "ch"),
            P("seq", "ch"),
            P("seq", "ch"),
            P("seq", "ch"),
            P(None, None, "ch"),
            P(None, "ch"),
            P("ch"),
        ),
        out_specs=(
            P("seq", "ch"),
            P("seq", "ch"),
            P("seq", "ch"),
            P("seq", "ch"),
            P(None, None, "ch"),
            P("ch"),
        ),
        check_vma=False,
    )
```

```python
import functools

import jax
import jax.numpy as jnp
import numpy as np
from jax import lax
from jax.experimental import pallas as pl
from jax.experimental.pallas import tpu as pltpu
from jax.sharding import PartitionSpec as P

F32 = jnp.float32
BF16 = jnp.bfloat16
ROWS = 16
VMEM_MIB = 52
UNROLL = 2


def transforms(span):
    freq = np.concatenate([np.arange(0, span, 2), np.arange(1, span, 2)]) + 0.5
    angle = np.pi * np.outer(freq, np.arange(span)) / span
    fwd = np.concatenate([np.cos(angle), -np.sin(angle)], 0)
    inv = fwd.T / span

    def halves(mat):
        mat = mat.astype(np.float32)
        high = mat.astype(jnp.bfloat16)
        low = (mat - high.astype(np.float32)).astype(jnp.bfloat16)
        return high, low

    fh, fl = halves(fwd)
    ih, il = halves(inv)
    return (
        np.concatenate([np.concatenate([fh, fh], 1), np.concatenate([fl, fl], 1)], 0),
        np.concatenate([ih, il], 0),
        np.concatenate([np.eye(span)[::-1]] * 2, 1).astype(jnp.bfloat16),
    )


def split(value):
    high = value.astype(BF16)
    low = (value - high.astype(F32)).astype(BF16)
    return high, low


def remote(src, dst, send, recv, target):
    return pltpu.make_async_remote_copy(
        src_ref=src,
        dst_ref=dst,
        send_sem=send,
        recv_sem=recv,
        device_id={"seq": target},
        device_id_type=pl.DeviceIdType.MESH,
    )


def kernel(
    size, length, span, ntap, pad,
    q_all, k_all, v_all, g_all, sf_hbm, lf_hbm, gain_hbm, fh_hbm, ih_hbm, flip_hbm,
    bq_ref, bk_ref, bv_ref, filt_ref, taps_ref, skip_ref,
    q_in, k_in, v_in, g_in, lf_in, sf_ref, gain_in, fh_ref, ih_ref, flip_ref,
    kx, vx, qx, gx, kf, vf, zf, gs, zh, zl, gh, gl, zw, gw, hw, sx, gz, prod, acc, part, gqs, gks, gvs, sums,
    kp_all, vp_all, qp_all, qn_all, gn_all, kn_all, vn_all,
    mine, theirs, chip, others, smine, stheirs, schip, sothers, half, other_half,
    load_sem, fix_sem, halo_send, halo_recv,
    pair_send, pair_recv, chip_send, chip_recv,
    spair_send, spair_recv, schip_send, schip_recv, last_send, last_recv,
):
    _, ncol, _, lane = zh.shape
    width = ncol * lane
    hlf = width // 2
    half_span = span // 2
    nblk = length // span
    big = span + pad
    tile = pl.program_id(0)
    tiles = kp_all.shape[0]
    chips = size // 2
    block = span // size
    me = lax.axis_index("seq")
    core = lax.rem(me, 2)
    place = me // 2
    partner = me + 1 - 2 * core

    def cols_of(t):
        return pl.ds(pl.multiple_of(t * width, width), width)

    def to_next(t):
        cols = cols_of(t)
        target = lax.rem(me + 1, size)
        parts = ((k_all, big, kp_all), (v_all, big, vp_all), (q_all, pad, qp_all))
        return [
            remote(src.at[pl.ds(length - rows, rows), cols], dst.at[t], halo_send.at[t, j], halo_recv.at[t, j], target)
            for j, (src, rows, dst) in enumerate(parts)
        ]

    def to_prev(t):
        cols = cols_of(t)
        target = lax.rem(me + size - 1, size)
        parts = ((q_all, big, qn_all), (g_all, big, gn_all), (k_all, pad, kn_all), (v_all, pad, vn_all))
        return [
            remote(src.at[pl.ds(0, rows), cols], dst.at[t], halo_send.at[t, 3 + j], halo_recv.at[t, 3 + j], target)
            for j, (src, rows, dst) in enumerate(parts)
        ]

    def pair_copy(t):
        return remote(mine.at[t, 1 - core], theirs.at[t], pair_send.at[t], pair_recv.at[t], partner)

    def chip_copy(t, d):
        there = lax.rem(place + d, chips)
        return remote(chip.at[t, there], others.at[t, d], chip_send.at[t, d], chip_recv.at[t, d], there * 2 + core)

    def spair_copy(t):
        return remote(smine.at[t, 1 - core], stheirs.at[t], spair_send.at[t], spair_recv.at[t], partner)

    def schip_copy(t, d):
        there = lax.rem(place + d, chips)
        return remote(schip.at[t], sothers.at[t, d], schip_send.at[t, d], schip_recv.at[t, d], there * 2 + core)

    def last_copy():
        return remote(half, other_half, last_send, last_recv, partner)

    def loads(t):
        cols = cols_of(t)
        pairs = ((k_all, k_in), (v_all, v_in), (q_all, q_in), (g_all, g_in))
        out = [pltpu.make_async_copy(lf_hbm.at[:, cols], lf_in.at[:, cols], load_sem.at[t, 0])]
        for j, (a, b) in enumerate(pairs):
            for c in range(ncol):
                strip = pl.ds(pl.multiple_of(t * width + c * lane, lane), lane)
                out.append(pltpu.make_async_copy(a.at[:, strip], b.at[t * ncol + c], load_sem.at[t, 1 + j * ncol + c]))
        return out

    def fixed():
        pairs = ((sf_hbm, sf_ref), (fh_hbm, fh_ref), (ih_hbm, ih_ref), (flip_hbm, flip_ref), (gain_hbm, gain_in))
        return [pltpu.make_async_copy(a, b, fix_sem.at[j]) for j, (a, b) in enumerate(pairs)]

    @pl.when(tile == 0)
    def _():
        barrier = pltpu.get_barrier_semaphore()
        for d in range(1, size):
            pl.semaphore_signal(
                barrier, inc=1, device_id={"seq": lax.rem(me + d, size)}, device_id_type=pl.DeviceIdType.MESH
            )
        for copy in loads(0) + fixed():
            copy.start()
        pl.semaphore_wait(barrier, size - 1)

        def send(t, _):
            @pl.when(me < size - 1)
            def _():
                for copy in to_next(t):
                    copy.start()

            @pl.when(me > 0)
            def _():
                for copy in to_prev(t):
                    copy.start()

            return 0

        lax.fori_loop(0, tiles, send, 0)

        def fetch(t, _):
            for copy in loads(t):
                copy.start()
            return 0

        lax.fori_loop(1, tiles, fetch, 0)

        @pl.when(me == 0)
        def _():
            for ref in (kp_all, vp_all, qp_all):
                ref[...] = jnp.zeros_like(ref)

        @pl.when(me == size - 1)
        def _():
            for ref in (qn_all, gn_all, kn_all, vn_all):
                ref[...] = jnp.zeros_like(ref)

        for copy in fixed():
            copy.wait()

    kp_ref, vp_ref, qp_ref = kp_all.at[tile], vp_all.at[tile], qp_all.at[tile]
    qn_ref, gn_ref, kn_ref, vn_ref = qn_all.at[tile], gn_all.at[tile], kn_all.at[tile], vn_all.at[tile]

    def join_long(t):
        pair_copy(t).wait_recv()
        chip[t] = mine[t, core] + theirs[t]
        others[t, 0] = mine[t, core, place] + theirs[t, place]
        for d in range(1, chips):
            chip_copy(t, d).start()

    def join_small(t):
        spair_copy(t).wait_recv()
        total = smine[t, core] + stheirs[t]
        schip[t] = total
        sothers[t, 0] = total
        for d in range(1, chips):
            schip_copy(t, d).start()

    for copy in loads(tile):
        copy.wait()

    @pl.when(tile > 0)
    def _():
        join_long(tile - 1)

    @pl.when(tile > 1)
    def _():
        join_small(tile - 2)

    @pl.when(me > 0)
    def _():
        for copy in to_next(tile):
            copy.wait_recv()

    @pl.when(me < size - 1)
    def _():
        for copy in to_prev(tile):
            copy.wait_recv()

    def here(c):
        return pl.ds(pl.multiple_of(tile * width + c * lane, lane), lane)

    def cut(c):
        return slice(c * lane, (c + 1) * lane)

    def taps(which, c):
        return [jnp.broadcast_to(sf_ref[which, i : i + 1, here(c)], (ROWS, lane)) for i in range(ntap)]

    weights = [[taps(w, c) for c in range(ncol)] for w in range(3)]

    def conv(ref, c, row, first, w):
        total = w[c][0] * first
        for i in range(1, ntap):
            total = total + w[c][i] * ref[c, pl.ds(row - i, ROWS), :]
        return total

    def slot(b):
        return nblk if b < 0 else b

    def put(high, low, row, c, value):
        h, l = split(value)
        at = slot(row // span), c, pl.ds(row % span, ROWS)
        high[at] = h
        low[at] = l

    def make_z(row, c, a0, b0, keep_taps, keep_z, keep_split=True):
        a = conv(kx, c, row + big, a0, weights[1])
        b = conv(vx, c, row + big, b0, weights[2])
        z = a * b
        if keep_taps:
            kf[c, pl.ds(row, ROWS), :] = a
            vf[c, pl.ds(row, ROWS), :] = b
        if keep_z:
            zf[c, pl.ds(row - (length - span), ROWS), :] = z
        if keep_split:
            put(zh, zl, row, c, z)

    def make_g(row, c, q0, g0, keep_g, keep_split=True):
        g = g0 * conv(qx, c, row + pad, q0, weights[0])
        if keep_g:
            gs[c, pl.ds(row - length, ROWS), :] = g
        if keep_split:
            put(gh, gl, row, c, g)

    def own(row, c, keep_z):
        a0 = k_in[tile * ncol + c, pl.ds(row, ROWS), :].astype(F32)
        b0 = v_in[tile * ncol + c, pl.ds(row, ROWS), :].astype(F32)
        q0 = q_in[tile * ncol + c, pl.ds(row, ROWS), :].astype(F32)
        g0 = g_in[tile * ncol + c, pl.ds(row, ROWS), :].astype(F32)
        kx[c, pl.ds(row + big, ROWS), :] = a0
        vx[c, pl.ds(row + big, ROWS), :] = b0
        qx[c, pl.ds(row + pad, ROWS), :] = q0
        gx[c, pl.ds(row, ROWS), :] = g0
        make_z(row, c, a0, b0, True, keep_z)
        make_g(row, c, q0, g0, False)

    def wide(strips):
        return jnp.concatenate(list(strips), 1)

    def spectrum(high, low):
        both = jnp.dot(fh_ref[...], jnp.concatenate([high, low], 0), preferred_element_type=F32)
        return both[: 2 * span] + both[2 * span :]

    def forward(high, low, b, out):
        at = slot(b)
        out[...] = spectrum(wide(high[at, c] for c in range(ncol)), wide(low[at, c] for c in range(ncol)))

    gain = gain_in[:, cols_of(tile)]
    taps_h = lf_in[:, cols_of(tile)]
    first = lax.broadcasted_iota(jnp.int32, (span, width), 0) == 0
    hh, hl = split(taps_h + jnp.where(first, gain, 0.0))
    hw[...] = spectrum(hh, hl)
    for c in range(ncol):
        for ref, src, at in (
            (kx, kp_ref, 0), (vx, vp_ref, 0), (qx, qp_ref, 0),
            (kx, kn_ref, big + length), (vx, vn_ref, big + length), (qx, qn_ref, pad + length),
            (gx, gn_ref, length),
        ):
            ref[c, at : at + src.shape[0], :] = src[:, cut(c)].astype(F32)

    def own_block(b):
        for c in range(ncol):
            for r in range(span // ROWS):
                own(b * span + r * ROWS, c, b == nblk - 1)

    def rows_of(ref, c, row):
        return ref[c, row : row + ROWS, :]

    def forward_z(b):
        forward(zh, zl, b, zw.at[b + 1])

    def forward_g(b):
        forward(gh, gl, b, gw.at[b])

    mid = nblk // 2
    for b in range(nblk):
        own_block(b)
        if b >= mid - 1:
            forward_z(b)
        if b >= mid:
            forward_g(b)
    for c in range(ncol):
        for r in range(span // ROWS + 1):
            row = length + r * ROWS
            make_g(row, c, rows_of(qx, c, row + pad), rows_of(gx, c, row), True, r < span // ROWS)
        row = length
        make_z(row, c, rows_of(kx, c, row + big), rows_of(vx, c, row + big), True, True, False)
    forward_g(nblk)
    for c in range(ncol):
        for r in range(span // ROWS):
            row = r * ROWS - span
            make_z(row, c, rows_of(kx, c, row + big), rows_of(vx, c, row + big), False, False)
    for b in range(mid - 1, -2, -1):
        if b < mid - 1:
            forward_z(b)
        if b >= 0:
            forward_g(b)
    back_h = jnp.dot(flip_ref[...], jnp.concatenate(split(taps_h), 0), preferred_element_type=F32)
    line = lax.broadcasted_iota(jnp.int32, (8, lane), 0)
    for c in range(ncol):
        edge_s = jnp.zeros((8, lane), F32)
        edge_z = jnp.zeros((8, lane), F32)
        for i in range(ntap - 1):
            zrow = zf[c, span + i : span + i + 1, :]
            grow = gs[c, i : i + 1, :]
            win = zf[c, i + 1 : i + 1 + span, :]
            value = jnp.sum(win * back_h[:, cut(c)], axis=0, keepdims=True) + gain[:, cut(c)] * zrow
            edge_s = jnp.where(line == i, value, edge_s)
            win = gs[c, i : i + span, :]
            value = jnp.sum(win * taps_h[:, cut(c)], axis=0, keepdims=True) + gain[:, cut(c)] * grow
            edge_z = jnp.where(line == i, value, edge_z)
        gqs[c, length : length + 8, :] = gx[c, length : length + 8, :] * edge_s
        gks[c, length : length + 8, :] = edge_z * vf[c, length : length + 8, :]
        gvs[c, length : length + 8, :] = edge_z * kf[c, length : length + 8, :]

    steps = span // ROWS * ncol

    def product(blocks, sign, n, _):
        if isinstance(n, int):
            re, im = pl.ds(n // ncol * ROWS, ROWS), pl.ds(n // ncol * ROWS + span, ROWS)
            pc = n % ncol
            col = cut(pc)
        else:
            fr = pl.multiple_of(n // ncol * ROWS, ROWS)
            re, im = pl.ds(fr, ROWS), pl.ds(fr + span, ROWS)
            pc = lax.rem(n, ncol)
            col = pl.ds(pl.multiple_of(pc * lane, lane), lane)

        def store(at, rows, value):
            h, l = split(value)
            prod[at, 0, pc, rows, :] = h
            prod[at, 1, pc, rows, :] = l

        hr, hi = hw[re, col], hw[im, col]
        b = blocks[0]
        zr, zi = zw[b, re, col], zw[b, im, col]
        gr, gi = gw[b, re, col], gw[b, im, col]
        ar = ai = None
        if b == 0:
            ar, ai = acc[re, col], acc[im, col]
        for b in blocks:
            zr2, zi2 = zw[b + 1, re, col], zw[b + 1, im, col]
            gr2, gi2 = gw[b + 1, re, col], gw[b + 1, im, col]
            if sign > 0:
                yr, yi = zr2 - zi, zi2 + zr
                xr, xi = gr + gi2, gi - gr2
            else:
                yr, yi = zr2 + zi, zi2 - zr
                xr, xi = gr - gi2, gi + gr2
            store(2 * b, re, yr * hr - yi * hi)
            store(2 * b, im, yr * hi + yi * hr)
            store(2 * b + 1, re, xr * hr + xi * hi)
            store(2 * b + 1, im, xi * hr - xr * hi)
            tr, ti = gr * yr + gi * yi, gi * yr - gr * yi
            ar, ai = (tr, ti) if ar is None else (ar + tr, ai + ti)
            zr, zi, gr, gi = zr2, zi2, gr2, gi2
        if blocks[0] == 0:
            store(2 * nblk, re, ar)
            store(2 * nblk, im, ai)
        else:
            acc[re, col] = ar
            acc[im, col] = ai
        return 0

    late = range(nblk // 2, nblk)
    for n in range(steps):
        product(late, 1 if n < steps // 2 else -1, n, 0)

    def inverse(at, out):
        both = jnp.dot(ih_ref[...], wide(prod[at, 0, c] for c in range(ncol)), preferred_element_type=F32)
        rest = jnp.dot(ih_ref[:span], wide(prod[at, 1, c] for c in range(ncol)), preferred_element_type=F32)
        out[...] = both[:span] + both[span:] + rest


    def back_to_time(b):
        inverse(2 * b, sx.at[b % 2])
        inverse(2 * b + 1, gz.at[b % 2])

    back_to_time(nblk - 1)
    for n in range(steps):
        product(range(nblk // 2), 1 if n < steps // 2 else -1, n, 0)
    inverse(2 * nblk, part)
    for d in range(size):
        mine[tile, d % 2, d // 2] = part[d * block : (d + 1) * block]
    pair_copy(tile).start()

    def fold(value):
        total = value[:8]
        for r in range(8, ROWS, 8):
            total = total + value[r : r + 8]
        return total

    per = span // ROWS
    sums[...] = jnp.zeros_like(sums)

    def last(b):
        if b > 0:
            back_to_time(b - 1)
        for c in range(ncol):
            total = [[sums[w, i, :, cut(c)] for i in range(ntap)] for w in range(3)]
            for r in range(per):
                row = b * span + (per - 1 - r) * ROWS
                at = pl.ds(row, ROWS)
                inner = slice(row - b * span, row - b * span + ROWS)
                gzc = gz[b % 2, inner, cut(c)]
                grads = (gx[c, at, :] * sx[b % 2, inner, cut(c)], gzc * vf[c, at, :], gzc * kf[c, at, :])
                for w, (grad, ref, own_x, off, out) in enumerate(zip(
                    grads, (gqs, gks, gvs), (qx, kx, vx), (pad, big, big), (bq_ref, bk_ref, bv_ref)
                )):
                    ref[c, at, :] = grad
                    x = own_x[c, pl.ds(row + off, ROWS), :]
                    res = weights[w][c][0] * grad
                    total[w][0] = total[w][0] + fold(grad * x)
                    for i in range(1, ntap):
                        later = ref[c, pl.ds(row + i, ROWS), :]
                        res = res + weights[w][c][i] * later
                        total[w][i] = total[w][i] + fold(later * x)
                    out[tile * ncol + c, at, :] = res.astype(BF16)
            for w in range(3):
                for i in range(ntap):
                    sums[w, i, :, cut(c)] = total[w][i]

    for b in reversed(range(nblk)):
        last(b)
    rows = [jnp.sum(sums[w, i], axis=0, keepdims=True) for w in range(3) for i in range(ntap)]
    rows.append(part[0:1, :])
    small = jnp.concatenate(rows + [jnp.zeros((pad - len(rows), width), F32)], 0)
    for p in range(2):
        smine[tile, p] = small[:, p * hlf : (p + 1) * hlf]
    spair_copy(tile).start()

    @pl.when(tile == tiles - 1)
    def _():
        join_long(tiles - 1)
        for t in range(max(tiles - 2, 0), tiles):
            join_small(t)

        def finish(t, _):
            cols = cols_of(t)

            @pl.when(me < size - 1)
            def _():
                for copy in to_next(t):
                    copy.wait_send()

            @pl.when(me > 0)
            def _():
                for copy in to_prev(t):
                    copy.wait_send()

            pair_copy(t).wait_send()
            spair_copy(t).wait_send()
            for d in range(1, chips):
                chip_copy(t, d).wait_send()
                chip_copy(t, d).wait_recv()
                schip_copy(t, d).wait_send()
                schip_copy(t, d).wait_recv()
            total = others[t, place]
            small = sothers[t, place]
            for z in range(1, chips):
                d = lax.rem(place + chips - z, chips)
                total = total + others[t, d]
                small = small + sothers[t, d]
            filt_ref[:, cols] = total
            half[t] = small
            return 0

        lax.fori_loop(0, tiles, finish, 0)
        last_copy().start()
        last_copy().wait()

        def write(t, _):
            for p in range(2):
                own_half = half[t]
                total = jnp.where(core == p, own_half, other_half[t])
                cols = pl.ds(pl.multiple_of(t * width + p * hlf, hlf), hlf)
                for w in range(3):
                    for i in range(ntap):
                        at = w * ntap + i
                        taps_ref[w, i : i + 1, cols] = total[at : at + 1]
                skip_ref[:, cols] = total[3 * ntap : 3 * ntap + 1]
            return 0

        lax.fori_loop(0, tiles, write, 0)


def settle(*refs):
    half = len(refs) // 2
    sem = refs[-1]
    copies = []
    for src, dst in zip(refs[:half], refs[half:-1]):
        if src.shape == dst.shape:
            copies.append((src, dst))
        else:
            lane = src.shape[2]
            copies += [(src.at[n], dst.at[:, n * lane : (n + 1) * lane]) for n in range(src.shape[0])]
    copies = [pltpu.make_async_copy(src, dst, sem.at[n]) for n, (src, dst) in enumerate(copies)]
    for copy in copies:
        copy.start()
    for copy in copies:
        copy.wait()


def body(input_q, input_k, input_v, grad_out, short_filters, long_filter, skip_gain):
    length, channels = input_q.shape
    ntap = short_filters.shape[1]
    span = long_filter.shape[0]
    pad = 16
    lane = 128
    big = span + pad
    width = min(256, channels)
    mats = [jnp.asarray(m) for m in transforms(span)]
    nblk = length // span

    size = lax.axis_size("seq")
    tiles = channels // width
    chips = size // 2
    block = span // size
    ncol = width // lane
    cells = lambda *rows: pltpu.VMEM((*rows, width), F32)
    strips = lambda rows: pltpu.VMEM((ncol, rows, lane), F32)
    halves = lambda *rows: pltpu.VMEM((*rows, lane), BF16)
    edge = lambda rows: pltpu.VMEM((tiles, rows, width), BF16)
    small = lambda *lead: pltpu.VMEM((*lead, pad, width // 2), F32)
    dma = lambda *shape: pltpu.SemaphoreType.DMA(shape)
    whole = pl.BlockSpec(memory_space=pltpu.VMEM)
    outs = pl.pallas_call(
        functools.partial(kernel, size, length, span, ntap, pad),
        grid=(tiles,),
        out_shape=(
            *[pltpu.VMEM((tiles * ncol, length, lane), BF16) for _ in range(3)],
            pltpu.VMEM((block, channels), F32),
            pltpu.VMEM((3, ntap, channels), F32),
            pltpu.VMEM((1, channels), F32),
        ),
        in_specs=[pl.BlockSpec(memory_space=pltpu.HBM)] * 10,
        out_specs=(whole,) * 6,
        scratch_shapes=[
            *[pltpu.VMEM((tiles * ncol, length, lane), BF16) for _ in range(4)],
            pltpu.VMEM((span, channels), F32), pltpu.VMEM((3, ntap, channels), F32), pltpu.VMEM((1, channels), F32),
            *[pltpu.VMEM(m.shape, BF16) for m in mats],
            strips(length + big + pad), strips(length + big + pad), strips(length + big + pad), strips(length + big),
            strips(length + pad), strips(length + pad), strips(span + pad), strips(span + pad),
            *[halves(nblk + 1, ncol, span) for _ in range(4)],
            cells(nblk + 1, 2 * span), cells(nblk + 1, 2 * span), cells(2 * span), cells(2, span), cells(2, span),
            halves(2 * nblk + 1, 2, ncol, 2 * span), cells(2 * span), cells(span),
            strips(length + pad), strips(length + pad), strips(length + pad), cells(3, ntap, 8),
            edge(big), edge(big), edge(pad), edge(big), edge(big), edge(pad), edge(pad),
            cells(tiles, 2, chips, block), cells(tiles, chips, block),
            cells(tiles, chips, block), cells(tiles, chips, block),
            small(tiles, 2), small(tiles), small(tiles), small(tiles, chips), small(tiles), small(tiles),
            dma(tiles, 1 + 4 * ncol), dma(5), dma(tiles, 7), dma(tiles, 7),
            dma(tiles), dma(tiles), dma(tiles, chips), dma(tiles, chips),
            dma(tiles), dma(tiles), dma(tiles, chips), dma(tiles, chips),
            pltpu.SemaphoreType.DMA, pltpu.SemaphoreType.DMA,
        ],
        compiler_params=pltpu.CompilerParams(
            dimension_semantics=("arbitrary",),
            vmem_limit_bytes=VMEM_MIB * 1024 * 1024,
            collective_id=0,
            has_side_effects=True,
        ),
        name="hyena_back",
    )(input_q, input_k, input_v, grad_out, short_filters, long_filter, skip_gain[None], *mats)
    outs = [pltpu.with_memory_space_constraint(out, pltpu.VMEM) for out in outs]
    back_q, back_k, back_v, grad_filt, grad_taps, grad_gain = pl.pallas_call(
        settle,
        out_shape=tuple(
            jax.ShapeDtypeStruct((length, channels) if n < 3 else out.shape, out.dtype) for n, out in enumerate(outs)
        ),
        in_specs=[whole] * 6,
        out_specs=(pl.BlockSpec(memory_space=pltpu.HBM),) * 6,
        scratch_shapes=[dma(3 * tiles * ncol + 3)],
        compiler_params=pltpu.CompilerParams(vmem_limit_bytes=1024 * 1024),
        name="settle",
    )(*outs)
    return (back_q, back_k, back_v, grad_filt, grad_taps, grad_gain[0])


def solution(mesh):
    return jax.shard_map(
        body,
        mesh=mesh,
        in_specs=(
            P("seq", "ch"),
            P("seq", "ch"),
            P("seq", "ch"),
            P("seq", "ch"),
            P(None, None, "ch"),
            P(None, "ch"),
            P("ch"),
        ),
        out_specs=(
            P("seq", "ch"),
            P("seq", "ch"),
            P("seq", "ch"),
            P("seq", "ch"),
            P(None, None, "ch"),
            P("ch"),
        ),
        check_vma=False,
    )
```
